32 devices in a mesh: dp: 4 (over z), mp: 8 (over y, x, core).
Axes of the slice: x: 2, y: 2, z: 4, core: 2. Of those that a mesh axis runs over, the one named last changes fastest.
Arguments:
- grad_parts: bfloat16 [4, 8, 2, 18432, 128], P('dp', 'mp'), may hold values from -45 to 45
- master: float32 [8, 2, 18432, 128], P('mp', None, 'dp'), may hold values from -15 to 15
- momenta: float32 [3, 8, 2, 18432, 128], P(None, 'mp', None, 'dp'), may hold values from -45 to 45
- second: float32 [3, 8, 2, 18432, 128], P(None, 'mp', None, 'dp'), may hold values from 0.00025 to 330
- step_count: int32 [1], replicated, may hold values from 1 to 99999
- mlp_first: float32 [8, 4], replicated, may hold values from -2 to 2
- mlp_bias: float32 [4], replicated, may hold values from -3 to 3
- mlp_second: float32 [4, 2], replicated, may hold values from -3 to 3
- tensor_weight: float32 [10], replicated, may hold values from -2 to 2
Outputs:
- new_params: bfloat16 [8, 2, 18432, 128], P('mp')
- new_master: float32 [8, 2, 18432, 128], P('mp', None, 'dp')
- new_momenta: float32 [3, 8, 2, 18432, 128], P(None, 'mp', None, 'dp')
- new_second: float32 [3, 8, 2, 18432, 128], P(None, 'mp', None, 'dp')
- update: float32 [8, 2, 18432, 128], P('mp', None, 'dp')
The draws below stay inside these ranges and needn't reach their ends.
All inputs are finite; a program needn't handle non-finite values.
Results may differ from the reference program's by a relative error of at most 0.019.
Values may be sent and summed in bfloat16 or wider, within the bound.
A program may use at most 192 MiB of HBM per device.

```python
import jax
import jax.numpy as jnp
from jax import lax

D = 4608
HQ = 4096
LANES = 128
FEATS = 8
HIDDEN_UNITS = 4
NT = 2
ROWS = 18432
OWN = 4608
N_DP = 4
N_MP = 8


def texture(key):
    key_rows = jax.random.fold_in(key, 1)
    key_lanes = jax.random.fold_in(key, 2)
    key_blocks = jax.random.fold_in(key, 3)
    position = jnp.arange(N_MP, dtype=jnp.float32) / max(N_MP - 1, 1)
    rising = jnp.exp(jnp.log(3.0) * position)[:, None, None, None]
    owner = jnp.arange(N_DP, dtype=jnp.float32) / max(N_DP - 1, 1)
    owner_rise = jnp.exp(jnp.log(3.0) * (owner - 1.0))[None, None, :, None, None]
    owner_random = jnp.exp(jax.random.uniform(key_blocks, (N_MP, NT, N_DP, 1, 1), minval=-jnp.log(3.0), maxval=0.0))
    row_part = jnp.exp(jax.random.uniform(key_rows, (N_MP, NT, N_DP, OWN, 1), minval=0.0, maxval=jnp.log(5.0)))
    row_part = (row_part * owner_rise * owner_random).reshape(N_MP, NT, ROWS, 1)
    lane_part = jnp.exp(jax.random.uniform(key_lanes, (1, NT, 1, LANES), minval=0.0, maxval=jnp.log(2.0)))
    return rising * row_part * lane_part


def draw_grad_parts(key, part):
    scales = texture(jax.random.fold_in(key, 11))
    ratio = jnp.exp(jnp.log(3.0) * jnp.arange(N_DP, dtype=jnp.float32) / max(N_DP - 1, 1))[:, None, None, None, None]
    key_noise = jax.random.fold_in(key, 12)
    noise = jax.random.truncated_normal(key_noise, -5.0, 5.0, (N_DP, N_MP, NT, ROWS, LANES))
    values = 0.1 * ratio * scales * noise
    return values.astype(jnp.bfloat16)


def draw_master(key, part):
    scales = texture(jax.random.fold_in(key, 21))
    key_noise = jax.random.fold_in(key, 22)
    noise = jax.random.truncated_normal(key_noise, -5.0, 5.0, (N_MP, NT, ROWS, LANES))
    return 0.1 * scales * noise


def draw_momenta(key, part):
    scales = texture(jax.random.fold_in(key, 31))
    key_noise = jax.random.fold_in(key, 32)
    noise = jax.random.truncated_normal(key_noise, -5.0, 5.0, (3, N_MP, NT, ROWS, LANES))
    return 0.3 * scales[None] * noise


def draw_second(key, part):
    scales = texture(jax.random.fold_in(key, 41))
    key_noise = jax.random.fold_in(key, 42)
    factor = jnp.exp(jax.random.uniform(key_noise, (3, N_MP, NT, ROWS, LANES), minval=jnp.log(0.25), maxval=jnp.log(4.0)))
    base = 0.3 * scales
    return (base * base)[None] * factor


def centred(stream_key, extent, deviation, most, kind=jnp.bfloat16):
    result = jax.random.normal(stream_key, extent, jnp.float32) * deviation
    return jnp.minimum(jnp.maximum(result, -most), most).astype(kind)


def setup_inputs(seed: int = 0) -> dict:
    key_list = jax.random.split(jax.random.key(seed), 10)
    return {
        "grad_parts": draw_grad_parts(jax.random.fold_in(key_list[9], 71), 0),
        "master": draw_master(jax.random.fold_in(key_list[9], 71), 0),
        "momenta": draw_momenta(jax.random.fold_in(key_list[9], 71), 0),
        "second": draw_second(jax.random.fold_in(key_list[9], 71), 0),
        "step_count": jax.random.randint(key_list[4], (1,), 1, 100000).astype(jnp.int32),
        "mlp_first": centred(key_list[5], (FEATS, HIDDEN_UNITS), FEATS ** -0.5, 2.0, jnp.float32),
        "mlp_bias": centred(key_list[6], (HIDDEN_UNITS,), 0.5, 3.0, jnp.float32),
        "mlp_second": centred(key_list[7], (HIDDEN_UNITS, 2), HIDDEN_UNITS ** -0.5, 3.0, jnp.float32),
        "tensor_weight": centred(key_list[8], (FEATS + 2,), 0.3, 2.0, jnp.float32),
    }


RATES = (0.9, 0.99, 0.999)

def features_of(master, gradient, moments, squares):
    listing = [master, gradient, moments[0], moments[1], moments[2]]
    for slot_id in range(3):
        listing.append(moments[slot_id] / jnp.sqrt(squares[slot_id]))
    return listing

def perceptron(normed, boost, mlp_first, mlp_bias, mlp_second):
    direction = jnp.zeros_like(normed[0])
    magnitude = jnp.zeros_like(normed[0])
    for unit_id in range(mlp_first.shape[1]):
        active = mlp_first[0, unit_id] * normed[0]
        for feat_id in range(1, len(normed)):
            active = active + mlp_first[feat_id, unit_id] * normed[feat_id]
        active = jax.nn.relu(active + mlp_bias[unit_id])
        direction = direction + mlp_second[unit_id, 0] * active
        magnitude = magnitude + mlp_second[unit_id, 1] * active
    return direction * jnp.exp(0.5 * jnp.tanh(magnitude)) * boost

def tensor_boost(norms, step_count, tensor_weight):
    count = tensor_weight.shape[0] - 2
    step_value = step_count[0].astype(jnp.float32)
    first_phase = jnp.log1p(step_value) / 11.5
    second_phase = step_value / 100000.0
    logits = lax.optimization_barrier(jnp.sum(tensor_weight[:count, None] * jnp.log(norms), axis=0))
    logits = logits + tensor_weight[count] * first_phase + tensor_weight[count + 1] * second_phase
    return jnp.exp(jnp.tanh(logits))

def reference(grad_parts, master, momenta, second, step_count, mlp_first, mlp_bias, mlp_second, tensor_weight):
    gradient = lax.optimization_barrier(jnp.sum(grad_parts, axis=0, dtype=jnp.float32))
    new_momenta = jnp.stack([rate * momenta[i] + (1.0 - rate) * gradient for i, rate in enumerate(RATES)])
    new_second = jnp.stack([rate * second[i] + (1.0 - rate) * gradient * gradient for i, rate in enumerate(RATES)])
    listing = features_of(master, gradient, new_momenta, new_second)
    totals = jnp.stack([lax.optimization_barrier(jnp.sum(feature * feature, axis=(0, 2, 3))) for feature in listing])
    norms = jnp.sqrt(totals / float(D * HQ) + 1e-06)
    boost = tensor_boost(norms, step_count, tensor_weight)[None, :, None, None]
    normed = [listing[i] / norms[i][None, :, None, None] for i in range(len(listing))]
    update = perceptron(normed, boost, mlp_first, mlp_bias, mlp_second)
    new_master = master - 0.05 * update
    new_params = new_master.astype(jnp.bfloat16)
    return (new_params, new_master, new_momenta, new_second, update)
```

```python
import functools

import jax
import jax.numpy as jnp
from jax import lax
from jax.experimental import pallas as pl
from jax.experimental.pallas import tpu as pltpu
from jax.sharding import PartitionSpec as P

D = 4608
HQ = 4096
RATES = (0.9, 0.99, 0.999)
MESH = pl.DeviceIdType.MESH
STRIP = 32


def block_rows(rows, most=1152):
    best = STRIP
    for size in range(STRIP, most + 1, STRIP):
        if rows % size == 0:
            best = size
    return best


def advanced(g, momenta, second):
    moments = [b * m + (1.0 - b) * g for b, m in zip(RATES, momenta)]
    gg = g * g
    squares = [b * s + (1.0 - b) * gg for b, s in zip(RATES, second)]
    return moments, squares


def listing_of(master, g, moments, squares):
    ratios = [m * lax.rsqrt(s) for m, s in zip(moments, squares)]
    return [master, g, *moments, *ratios]


def update_of(listing, coef, base, feats, hidden):
    direction = None
    magnitude = None
    tail = base + feats * hidden
    for j in range(hidden):
        active = listing[0] * coef[base + j] + coef[tail + j]
        for f in range(1, feats):
            active = active + listing[f] * coef[base + f * hidden + j]
        active = jnp.maximum(active, 0.0)
        d = active * coef[tail + hidden + j]
        m = active * coef[tail + 2 * hidden + j]
        direction = d if direction is None else direction + d
        magnitude = m if magnitude is None else magnitude + m
    return direction * jnp.exp(0.5 * jnp.tanh(magnitude))


def stats_kernel(steps, g_ref, master_ref, mom_ref, sec_ref, *rest):
    out_ref, acc = rest[-2:]
    i = pl.program_id(0)

    @pl.when(i == 0)
    def _():
        acc[...] = jnp.zeros_like(acc)

    def body(k, carry):
        rows = pl.ds(pl.multiple_of(k * STRIP, STRIP), STRIP)
        g = g_ref[rows, :].astype(jnp.float32)
        moments, squares = advanced(
            g, [mom_ref[c, 0, 0, rows, :] for c in range(3)], [sec_ref[c, 0, 0, rows, :] for c in range(3)]
        )
        feats = listing_of(master_ref[0, 0, rows, :], g, moments, squares)
        return tuple(
            a + jnp.sum((f * f).reshape(STRIP // 8, 8, 128), axis=0) for a, f in zip(carry, feats)
        )

    sums = lax.fori_loop(0, g_ref.shape[0] // STRIP, body, tuple(acc[f] for f in range(8)))
    for f in range(8):
        acc[f] = sums[f]

    @pl.when(i == steps - 1)
    def _():
        for f in range(8):
            out_ref[pl.ds(f, 1), :] = jnp.sum(acc[f], axis=0, keepdims=True)


def state_specs(rows, t_of):
    return [
        pl.BlockSpec((1, 1, rows, 128), lambda *a: (0, t_of(a), a[-1], 0)),
        pl.BlockSpec((3, 1, 1, rows, 128), lambda *a: (0, 0, t_of(a), a[-1], 0)),
        pl.BlockSpec((3, 1, 1, rows, 128), lambda *a: (0, 0, t_of(a), a[-1], 0)),
    ]


def cost(elements, flops, nbytes):
    return pl.CostEstimate(flops=elements * flops, bytes_accessed=nbytes, transcendentals=5 * elements)


def stats(t, g, master, momenta, second, after=()):
    own = g.shape[0]
    rows = block_rows(own)
    steps = own // rows
    return pl.pallas_call(
        functools.partial(stats_kernel, steps),
        grid=(steps,),
        out_shape=jax.ShapeDtypeStruct((8, 128), jnp.float32),
        in_specs=[pl.BlockSpec((rows, 128), lambda i: (i, 0))] + state_specs(rows, lambda a: t)
        + [pl.BlockSpec(memory_space=pl.ANY)] * len(after),
        out_specs=pl.BlockSpec((8, 128), lambda i: (0, 0)),
        scratch_shapes=[pltpu.VMEM((8, 8, 128), jnp.float32)],
        cost_estimate=cost(own * 128, 40, own * 128 * 30),
        name=f"stats{t}",
    )(g, master, momenta, second, *after)


def params_kernel(feats, hidden, coef, g_ref, master_ref, mom_ref, sec_ref, out_ref):
    def body(k, carry):
        rows = pl.ds(pl.multiple_of(k * STRIP, STRIP), STRIP)
        g = g_ref[rows, :].astype(jnp.float32)
        moments, squares = advanced(
            g, [mom_ref[c, 0, 0, rows, :] for c in range(3)], [sec_ref[c, 0, 0, rows, :] for c in range(3)]
        )
        master = master_ref[0, 0, rows, :]
        update = update_of(listing_of(master, g, moments, squares), coef, 0, feats, hidden)
        out_ref[rows, :] = (master - 0.05 * update).astype(jnp.bfloat16)
        return carry

    lax.fori_loop(0, g_ref.shape[0] // STRIP, body, 0)


def params(t, feats, hidden, coef, g, master, momenta, second):
    own = g.shape[0]
    rows = block_rows(own)
    return pl.pallas_call(
        functools.partial(params_kernel, feats, hidden),
        grid=(own // rows,),
        out_shape=jax.ShapeDtypeStruct((own, 128), jnp.bfloat16),
        in_specs=[pl.BlockSpec(memory_space=pltpu.SMEM), pl.BlockSpec((rows, 128), lambda i: (i, 0))]
        + state_specs(rows, lambda a: t),
        out_specs=pl.BlockSpec((rows, 128), lambda i: (i, 0)),
        cost_estimate=cost(own * 128, 130, own * 128 * 32),
        name=f"params{t}",
    )(coef, g, master, momenta, second)


def finish_kernel(
    feats, hidden, width, coef, g0_ref, g1_ref, master_ref, mom_ref, sec_ref, nm_ref, nmom_ref, nsec_ref, up_ref
):
    t = pl.program_id(0)
    base = t * width

    def body(k, carry):
        rows = pl.ds(pl.multiple_of(k * STRIP, STRIP), STRIP)
        g = jnp.where(t == 0, g0_ref[rows, :].astype(jnp.float32), g1_ref[rows, :].astype(jnp.float32))
        moments, squares = advanced(
            g, [mom_ref[c, 0, 0, rows, :] for c in range(3)], [sec_ref[c, 0, 0, rows, :] for c in range(3)]
        )
        for c in range(3):
            nmom_ref[c, 0, 0, rows, :] = moments[c]
            nsec_ref[c, 0, 0, rows, :] = squares[c]
        master = master_ref[0, 0, rows, :]
        update = update_of(listing_of(master, g, moments, squares), coef, base, feats, hidden)
        up_ref[0, 0, rows, :] = update
        nm_ref[0, 0, rows, :] = master - 0.05 * update
        return carry

    lax.fori_loop(0, g0_ref.shape[0] // STRIP, body, 0)


def finish(feats, hidden, coefs, g0, g1, master, momenta, second):
    own = g0.shape[0]
    rows = block_rows(own)
    steps = own // rows
    width = coefs.shape[0] // 2
    specs = state_specs(rows, lambda a: a[0])
    return pl.pallas_call(
        functools.partial(finish_kernel, feats, hidden, width),
        grid=(2, steps),
        out_shape=(
            jax.ShapeDtypeStruct(master.shape, jnp.float32),
            jax.ShapeDtypeStruct(momenta.shape, jnp.float32),
            jax.ShapeDtypeStruct(second.shape, jnp.float32),
            jax.ShapeDtypeStruct(master.shape, jnp.float32),
        ),
        in_specs=[
            pl.BlockSpec(memory_space=pltpu.SMEM),
            pl.BlockSpec((rows, 128), lambda t, i: (i * (1 - t) + (steps - 1) * t, 0)),
            pl.BlockSpec((rows, 128), lambda t, i: (i * t, 0)),
        ]
        + specs,
        out_specs=(specs[0], specs[1], specs[2], specs[0]),
        cost_estimate=cost(2 * own * 128, 130, 2 * own * 128 * 62),
        name="finish",
    )(coefs, g0, g1, master, momenta, second)


def total_kernel(n_dp, n_mp, x_ref, out_ref, near, far, send1, recv1, send2, recv2, local_sem):
    z = lax.axis_index("dp")
    m = lax.axis_index("mp")
    mine = pltpu.make_async_copy(x_ref, near.at[0], local_sem)
    mine.start()
    barrier = pltpu.get_barrier_semaphore()
    for j in range(1, n_mp):
        pl.semaphore_signal(barrier, inc=1, device_id=(z, lax.rem(m + j, n_mp)), device_id_type=MESH)
    for j in range(1, n_dp):
        pl.semaphore_signal(barrier, inc=1, device_id=(lax.rem(z + j, n_dp), m), device_id_type=MESH)
    pl.semaphore_wait(barrier, n_mp - 1 + n_dp - 1)
    first = []
    for j in range(1, n_mp):
        copy = pltpu.make_async_remote_copy(
            src_ref=x_ref,
            dst_ref=near.at[j],
            send_sem=send1.at[j],
            recv_sem=recv1.at[j],
            device_id=(z, lax.rem(m + j, n_mp)),
            device_id_type=MESH,
        )
        copy.start()
        first.append(copy)
    mine.wait()
    for copy in first:
        copy.wait()
    second = []
    for j in range(1, n_dp):
        copy = pltpu.make_async_remote_copy(
            src_ref=near,
            dst_ref=far.at[j - 1],
            send_sem=send2.at[j],
            recv_sem=recv2.at[j],
            device_id=(lax.rem(z + j, n_dp), m),
            device_id_type=MESH,
        )
        copy.start()
        second.append(copy)
    for copy in second:
        copy.wait()
    total = jnp.sum(near[...], axis=0)
    for j in range(n_dp - 1):
        total = total + jnp.sum(far[j], axis=0)
    out_ref[...] = total


def total(which, n_dp, n_mp, x):
    return pl.pallas_call(
        functools.partial(total_kernel, n_dp, n_mp),
        out_shape=jax.ShapeDtypeStruct(x.shape, x.dtype),
        in_specs=[pl.BlockSpec(memory_space=pltpu.VMEM)],
        out_specs=pl.BlockSpec(memory_space=pltpu.VMEM),
        scratch_shapes=[
            pltpu.VMEM((n_mp,) + x.shape, x.dtype),
            pltpu.VMEM((n_dp - 1, n_mp) + x.shape, x.dtype),
            pltpu.SemaphoreType.DMA((n_mp,)),
            pltpu.SemaphoreType.DMA((n_mp,)),
            pltpu.SemaphoreType.DMA((n_dp,)),
            pltpu.SemaphoreType.DMA((n_dp,)),
            pltpu.SemaphoreType.DMA,
        ],
        compiler_params=pltpu.CompilerParams(collective_id=which, has_side_effects=True),
        cost_estimate=pl.CostEstimate(flops=1000, bytes_accessed=10_000_000, transcendentals=0),
        name=f"total{which}",
    )(x)


def coef_kernel(totals_ref, step_ref, first_ref, bias_ref, second_ref, weight_ref, out_ref):
    feats, hidden = first_ref.shape
    sums = jnp.sum(totals_ref[...], axis=1, keepdims=True) + jnp.zeros((feats, 128), jnp.float32)
    norms = jnp.sqrt(sums / float(D * HQ) + 1e-06)
    logs = jnp.log(norms)
    inverse = 1.0 / norms
    step = jnp.full((1, 128), step_ref[0].astype(jnp.float32))
    logits = weight_ref[feats] * (jnp.log(1.0 + step) / 11.5) + weight_ref[feats + 1] * (step / 100000.0)
    for f in range(feats):
        logits = logits + weight_ref[f] * logs[f : f + 1, :]
    boost = jnp.exp(jnp.tanh(logits))[0, 0]
    for f in range(feats):
        scale = inverse[f, 0]
        for j in range(hidden):
            out_ref[f * hidden + j] = first_ref[f, j] * scale
    tail = feats * hidden
    for j in range(hidden):
        out_ref[tail + j] = bias_ref[j]
        out_ref[tail + hidden + j] = second_ref[j, 0] * boost
        out_ref[tail + 2 * hidden + j] = second_ref[j, 1]


def coefficients(totals, step_count, mlp_first, mlp_bias, mlp_second, tensor_weight):
    feats, hidden = mlp_first.shape
    smem = pl.BlockSpec(memory_space=pltpu.SMEM)
    return pl.pallas_call(
        coef_kernel,
        out_shape=jax.ShapeDtypeStruct(((feats + 3) * hidden,), jnp.float32),
        in_specs=[pl.BlockSpec(memory_space=pltpu.VMEM)] + [smem] * 5,
        out_specs=smem,
        name="coefficients",
    )(totals, step_count, mlp_first, mlp_bias, mlp_second, tensor_weight)


def pick_kernel(x_ref, out_ref):
    out_ref[...] = x_ref[0, 0, 0]


def pick(t, grad_parts):
    total_rows = grad_parts.shape[3]
    rows = block_rows(total_rows, 4608)
    return pl.pallas_call(
        pick_kernel,
        grid=(total_rows // rows,),
        out_shape=jax.ShapeDtypeStruct(grad_parts.shape[3:], grad_parts.dtype),
        in_specs=[pl.BlockSpec((1, 1, 1, rows, 128), lambda i: (0, 0, t, i, 0))],
        out_specs=pl.BlockSpec((rows, 128), lambda i: (i, 0)),
        cost_estimate=pl.CostEstimate(flops=0, bytes_accessed=4 * total_rows * 128, transcendentals=0),
        name=f"pick{t}",
    )(grad_parts)


def local(
    n_dp, n_mp, grad_parts, master, momenta, second, step_count, mlp_first, mlp_bias, mlp_second, tensor_weight
):
    feats, hidden = mlp_first.shape
    net = (step_count, mlp_first, mlp_bias, mlp_second, tensor_weight)
    g0 = lax.psum_scatter(pick(0, grad_parts), "dp", scatter_dimension=0, tiled=True)
    g0, part1 = lax.optimization_barrier((g0, pick(1, grad_parts)))
    g1 = lax.psum_scatter(part1, "dp", scatter_dimension=0, tiled=True)
    coef0 = coefficients(total(0, n_dp, n_mp, stats(0, g0, master, momenta, second)), *net)
    p0 = params(0, feats, hidden, coef0, g0, master, momenta, second)
    full0 = lax.all_gather(p0, "dp", axis=0, tiled=True)
    coef1 = coefficients(total(1, n_dp, n_mp, stats(1, g1, master, momenta, second, (p0,))), *net)
    p1 = params(1, feats, hidden, coef1, g1, master, momenta, second)
    full1 = lax.all_gather(p1, "dp", axis=0, tiled=True)
    new_master, new_momenta, new_second, update = finish(
        feats, hidden, jnp.concatenate([coef0, coef1]), g0, g1, master, momenta, second
    )
    out = jnp.stack([full0, full1])[None]
    return (out, new_master, new_momenta, new_second, update)


def solution(mesh):
    placed = (
        P("dp", "mp", None, None, None),
        P("mp", None, "dp", None),
        P(None, "mp", None, "dp", None),
        P(None, "mp", None, "dp", None),
        P(),
        P(),
        P(),
        P(),
        P(),
    )
    return jax.shard_map(
        functools.partial(local, mesh.shape["dp"], mesh.shape["mp"]),
        mesh=mesh,
        in_specs=placed,
        out_specs=(
            P("mp", None, None, None),
            P("mp", None, "dp", None),
            P(None, "mp", None, "dp", None),
            P(None, "mp", None, "dp", None),
            P("mp", None, "dp", None),
        ),
        check_vma=False,
    )
```
